32 devices in a mesh: dom: 32 (over z, y, x, core).
Axes of the slice: x: 2, y: 2, z: 4, core: 2. Of those that a mesh axis runs over, the one named last changes fastest.
Arguments:
- forcing: float32 [1024, 128], P('dom'), may hold values from -6 to 6
- first_guess: float32 [1024, 128], P('dom'), may hold values from -4 to 4
- corners: int32 [3, 262144], P(None, 'dom'), may hold values from 0 to 8191, as said below
- gradients: float32 [4, 262144], P(None, 'dom'), may hold values from -5 to 5
- element_area: float32 [262144], P('dom'), may hold values from 0.5 to 2
- element_depth: float32 [262144], P('dom'), may hold values from 0.2 to 4
- send_blocks: int32 [32, 4, 8], P('dom'), may hold values from 0 to 32, as said below
- recv_blocks: int32 [32, 4, 8], P('dom'), may hold values from 0 to 32, as said below
Outputs:
- elevation: float32 [1024, 128], P('dom')
- residual_left: float32 [1024, 128], P('dom')
The draws below stay inside these ranges and needn't reach their ends.
Inputs may be any that keep to these rules, and one draw needn't show every extreme that they name: `corners`: column e of device d's elements names three different local nodes of device d, numbered below (64) * 128: numbers below 4096 are its owned nodes in block order, the rest its halo blocks. The first corner is an owned node, and every owned node is the first corner of some element of its device. `send_blocks`: entry [d, o, s] is the owned block of device d sent in slot s of offset o to the reader d - k_o, or 32 for an empty slot; it is live exactly when recv_blocks[d - k_o, o, s] is, and readers outside the mesh get nothing. Live blocks of one device and offset differ. For k_o = 1 every slot toward an existing reader is live. `recv_blocks`: entry [q, o, s] is the halo block of device q filled by slot s of offset o from device q + k_o, or 32 for an empty slot. The live entries of one device differ.
All inputs are finite; a program needn't handle non-finite values.
Results may differ from the reference program's by a relative error of at most 0.00022.
Values sent between devices are 32-bit elements; how exact they have to be, the bound alone decides.
A program may use at most 64 MiB of HBM per device.

```python
import math
import jax
import jax.numpy as jnp

BLOCK = 128
OWN_BLOCKS = 32
SLOTS = 8
REACH = 2
ITERS = 2
OFFSETS = 4
HALO_BLOCKS = 32
ELEM_DEV = 8192
NODES = 131072
ELEMS = 262144
N_DOM = 32


def shift_values():
    return jnp.array([shift_at - REACH if shift_at < REACH else shift_at - REACH + 1 for shift_at in range(OFFSETS)], dtype=jnp.int32)


def link_tables(key):
    base = jax.random.fold_in(key, 4242)
    key_live, key_start, key_place = jax.random.split(base, 3)
    shift_table = shift_values()
    readers = jnp.arange(N_DOM, dtype=jnp.int32)[:, None, None]
    sources = readers + shift_table[None, :, None]
    inside = (sources >= 0) & (sources < N_DOM)
    coin = jax.random.randint(key_live, (N_DOM, OFFSETS, SLOTS), 0, 4, dtype=jnp.int32)
    forced = jnp.broadcast_to(shift_table[None, :, None] == 1, (N_DOM, OFFSETS, SLOTS))
    live = inside & ((coin != 0) | forced)
    start = jax.random.randint(key_start, (N_DOM, OFFSETS, 1), 0, OWN_BLOCKS, dtype=jnp.int32)
    slot_ids = jnp.arange(SLOTS, dtype=jnp.int32)[None, None, :]
    read_blocks = jnp.where(live, (start + slot_ids) % OWN_BLOCKS, OWN_BLOCKS).astype(jnp.int32)

    def placing(one_key):
        return jax.random.permutation(one_key, HALO_BLOCKS)
    places = jax.vmap(placing)(jax.random.split(key_place, N_DOM)).astype(jnp.int32)
    places = places.reshape(N_DOM, OFFSETS, SLOTS)
    recv_table = jnp.where(live, places, HALO_BLOCKS).astype(jnp.int32)
    owners = jnp.arange(N_DOM, dtype=jnp.int32)[:, None, None]
    targets = owners - shift_table[None, :, None]
    target_in = (targets >= 0) & (targets < N_DOM)
    clipped = jnp.clip(targets, 0, N_DOM - 1).astype(jnp.int32)
    offset_ids = jnp.arange(OFFSETS, dtype=jnp.int32)[None, :, None]
    picked = read_blocks[clipped, offset_ids, slot_ids]
    send_table = jnp.where(target_in, picked, OWN_BLOCKS).astype(jnp.int32)
    return (send_table, recv_table)


def draw_send_blocks(key, part):
    return link_tables(key)[0]


def draw_recv_blocks(key, part):
    return link_tables(key)[1]


def draw_corners(key, part):
    base = jax.random.fold_in(key, 31)
    key_perm, key_first, key_second = jax.random.split(base, 3)
    owned_nodes = OWN_BLOCKS * BLOCK
    local_nodes = (OWN_BLOCKS + HALO_BLOCKS) * BLOCK

    def shuffled(one_key):
        return jax.random.permutation(one_key, ELEM_DEV)
    leading = jax.vmap(shuffled)(jax.random.split(key_perm, N_DOM)).astype(jnp.int32) % owned_nodes
    step_one = jax.random.randint(key_first, (N_DOM, ELEM_DEV), 1, local_nodes, dtype=jnp.int32)
    extra = jax.random.randint(key_second, (N_DOM, ELEM_DEV), 0, local_nodes - 2, dtype=jnp.int32)
    step_two = 1 + (step_one + extra) % (local_nodes - 1)
    stacked = jnp.stack([leading, (leading + step_one) % local_nodes, (leading + step_two) % local_nodes])
    return stacked.reshape(3, N_DOM * ELEM_DEV).astype(jnp.int32)


def block_scale(stream_key, shape, shards, least, top_value):
    factor_of = 1.0
    for axis_at, parts in shards:
        steps = jax.random.uniform(jax.random.fold_in(jax.random.fold_in(stream_key, 6), axis_at), (parts,), jnp.float32, least / len(shards), top_value / len(shards))
        factor_of = factor_of * jnp.repeat(jnp.exp(steps), shape[axis_at] // parts).reshape((-1,) + (1,) * (len(shape) - 1 - axis_at))
    return factor_of


def noise(own_key, dims, spread, reach, shards=(), kind=jnp.bfloat16):
    values = jax.random.normal(own_key, dims, jnp.float32) * spread
    if len(shards) > 0:
        values = block_scale(own_key, dims, shards, -0.22, 0.18) * values
    return jnp.clip(values, min=-reach, max=reach).astype(kind)


def setup_inputs(seed: int = 0) -> dict:
    arg_keys = jax.random.split(jax.random.key(seed), 9)
    return {
        "forcing": noise(arg_keys[0], (N_DOM * OWN_BLOCKS, BLOCK), 1.0, 6.0, ((0, 32),), jnp.float32),
        "first_guess": noise(arg_keys[1], (N_DOM * OWN_BLOCKS, BLOCK), 0.5, 4.0, ((0, 32),), jnp.float32),
        "corners": draw_corners(jax.random.fold_in(arg_keys[8], 71), 0),
        "gradients": noise(arg_keys[3], (4, ELEMS), 1.0, 5.0, ((1, 32),), jnp.float32),
        "element_area": jnp.clip(jnp.exp(math.log(2.0) - 1.3862944 * jax.random.uniform(arg_keys[4], (ELEMS,), jnp.float32) ** block_scale(arg_keys[4], (ELEMS,), ((0, 32),), -0.2, 0.2)), 0.5, 2.0),
        "element_depth": jnp.clip(jnp.exp(math.log(4.0) - 2.9957323 * jax.random.uniform(arg_keys[5], (ELEMS,), jnp.float32) ** block_scale(arg_keys[5], (ELEMS,), ((0, 32),), -0.2, 0.2)), 0.2, 4.0),
        "send_blocks": draw_send_blocks(jax.random.fold_in(arg_keys[8], 71), 0),
        "recv_blocks": draw_recv_blocks(jax.random.fold_in(arg_keys[8], 71), 0),
    }


def shift_list():
    return [shift_at - REACH if shift_at < REACH else shift_at - REACH + 1 for shift_at in range(OFFSETS)]


def node_numbers(corners, send_blocks, recv_blocks):
    shift_table = jnp.array(shift_list(), dtype=jnp.int32)
    readers = jnp.arange(N_DOM, dtype=jnp.int32)[:, None, None]
    sources = readers + shift_table[None, :, None]
    inside = (sources >= 0) & (sources < N_DOM)
    clipped = jnp.clip(sources, 0, N_DOM - 1).astype(jnp.int32)
    offset_ids = jnp.arange(OFFSETS, dtype=jnp.int32)[None, :, None]
    slot_ids = jnp.arange(SLOTS, dtype=jnp.int32)[None, None, :]
    source_block = send_blocks[clipped, offset_ids, slot_ids]
    live = inside & (source_block < OWN_BLOCKS) & (recv_blocks < HALO_BLOCKS)
    nowhere = N_DOM * OWN_BLOCKS
    global_block = jnp.where(live, clipped * OWN_BLOCKS + source_block, nowhere).astype(jnp.int32)
    target = jnp.where(live, recv_blocks, HALO_BLOCKS).astype(jnp.int32)
    readers_full = jnp.broadcast_to(readers, target.shape).astype(jnp.int32)
    halo_table = jnp.full((N_DOM, HALO_BLOCKS + 1), nowhere, dtype=jnp.int32)
    halo_table = halo_table.at[readers_full, target].set(global_block)
    owned_table = (jnp.arange(N_DOM, dtype=jnp.int32)[:, None] * OWN_BLOCKS
                   + jnp.arange(OWN_BLOCKS, dtype=jnp.int32)[None, :])
    block_table = jnp.concatenate([owned_table, halo_table[:, :HALO_BLOCKS]], axis=1)
    owners = (jnp.arange(N_DOM * ELEM_DEV, dtype=jnp.int32) // ELEM_DEV)[None, :]
    mapped = block_table[owners, corners // BLOCK]
    return (mapped * BLOCK + corners % BLOCK).astype(jnp.int32)


def reference(forcing, first_guess, corners, gradients, element_area, element_depth, send_blocks, recv_blocks):
    nodes = node_numbers(corners, send_blocks, recv_blocks)
    grad_x = [gradients[0], gradients[2], -(gradients[0] + gradients[2])]
    grad_y = [gradients[1], gradients[3], -(gradients[1] + gradients[3])]
    scaled = element_depth * element_area
    stiffness = [[scaled * (grad_x[row_at] * grad_x[col_at] + grad_y[row_at] * grad_y[col_at])
                  for col_at in range(3)] for row_at in range(3)]
    flat_nodes = nodes.reshape(-1)
    extent = NODES + BLOCK
    third = element_area / 3.0
    mass = jax.ops.segment_sum(jnp.concatenate([third, third, third]), flat_nodes,
                               num_segments=extent)[:NODES].reshape(forcing.shape)

    def operate(field):
        padded = jnp.concatenate([field.reshape(-1), jnp.zeros((BLOCK,), dtype=jnp.float32)])
        values = [padded[nodes[corner_at]] for corner_at in range(3)]
        contrib = jnp.concatenate([stiffness[row_at][0] * values[0] + stiffness[row_at][1] * values[1]
                                   + stiffness[row_at][2] * values[2] for row_at in range(3)])
        summed = jax.ops.segment_sum(contrib, flat_nodes, num_segments=extent)[:NODES].reshape(field.shape)
        return mass * field + summed

    elevation = first_guess
    residual = forcing - operate(first_guess)
    direction = residual
    norm_now = jnp.sum(residual * residual)
    for step_at in range(ITERS):
        applied = operate(direction)
        step_size = norm_now / jnp.sum(direction * applied)
        elevation = elevation + step_size * direction
        residual = residual - step_size * applied
        norm_next = jnp.sum(residual * residual)
        direction = residual + (norm_next / norm_now) * direction
        norm_now = norm_next
    return elevation, residual
```

```python
import functools

import jax
import jax.numpy as jnp
from jax import lax
from jax.experimental import pallas as pl
from jax.experimental.pallas import tpu as pltpu
from jax.sharding import PartitionSpec as P

LANES = 128
ROWS = 8


def shift_list(offsets):
    half_count = offsets // 2
    return [
        shift_at - half_count if shift_at < half_count else shift_at - half_count + 1
        for shift_at in range(offsets)
    ]


def kernel(
    n,
    forcing,
    guess,
    corners,
    gradients,
    area,
    depth,
    send,
    recv,
    elevation,
    residual,
    blk,
    lane,
    hot,
    elem,
    vals,
    hi,
    lo,
    field,
    halo_part,
    fwd_out,
    fwd_in,
    bwd_out,
    bwd_in,
    sum_out,
    sum_in,
    fwd_send_sem,
    fwd_recv_sem,
    bwd_send_sem,
    bwd_recv_sem,
    sum_send_sem,
    sum_recv_sem,
):
    own, _ = forcing.shape
    _, offsets, slots = send.shape
    halo = offsets * slots
    rows = area.shape[0]
    groups = rows // ROWS
    shifts = shift_list(offsets)
    me = lax.axis_index("dom")
    f32 = jnp.float32

    barrier = pltpu.get_barrier_semaphore()

    def greet(i, carry):
        pl.semaphore_signal(
            barrier, inc=1, device_id=(lax.rem(me + i, n),), device_id_type=pl.DeviceIdType.MESH
        )
        return carry

    lax.fori_loop(1, n, greet, 0)

    def there(distance):
        return jnp.logical_and(me + distance >= 0, me + distance < n)

    def fwd_copy(t, o):
        return pltpu.make_async_remote_copy(
            src_ref=fwd_out.at[t, o],
            dst_ref=fwd_in.at[t, o],
            send_sem=fwd_send_sem.at[t, o],
            recv_sem=fwd_recv_sem.at[t, o],
            device_id=(me - shifts[o],),
            device_id_type=pl.DeviceIdType.MESH,
        )

    def bwd_copy(t, o):
        return pltpu.make_async_remote_copy(
            src_ref=bwd_out.at[t, o],
            dst_ref=bwd_in.at[t, o],
            send_sem=bwd_send_sem.at[t, o],
            recv_sem=bwd_recv_sem.at[t, o],
            device_id=(me + shifts[o],),
            device_id_type=pl.DeviceIdType.MESH,
        )

    def when_there(distance, action):
        @pl.when(there(distance))
        def _():
            action()

    for o in range(offsets):

        @pl.when(jnp.logical_not(there(shifts[o])))
        def _():
            for t in range(3):
                fwd_in[t, o] = jnp.zeros((slots, LANES), f32)

        @pl.when(jnp.logical_not(there(-shifts[o])))
        def _():
            for t in range(3):
                bwd_in[t, o] = jnp.zeros((slots, LANES), f32)

    def pack(t, source):
        for o in range(offsets):
            for s in range(slots):
                at = jnp.minimum(send[0, o, s], own - 1)
                fwd_out[t, o, s : s + 1, :] = source[pl.ds(at, 1), :]

    def start_forward(t):
        for o in range(offsets):
            when_there(-shifts[o], lambda o=o: fwd_copy(t, o).start())

    pack(0, guess)
    pl.semaphore_wait(barrier, n - 1)
    start_forward(0)

    def lay(r, carry):
        at = pl.multiple_of(r * LANES, LANES)
        for c in range(3):
            lane[pl.ds(c * rows + r, 1), :] = corners[c : c + 1, pl.ds(at, LANES)]
        for c in range(4):
            elem[pl.ds(c * rows + r, 1), :] = gradients[c : c + 1, pl.ds(at, LANES)]
        return carry

    lax.fori_loop(0, rows, lay, 0)

    wide = lax.broadcasted_iota(jnp.int32, (ROWS, LANES), 1)
    table = jnp.where(wide < own, wide, 2 * LANES)
    for o in range(offsets):
        for s in range(slots):
            table = jnp.where(wide == own + recv[0, o, s], own + o * slots + s, table)
    table = jnp.where(wide < own + halo, table, 2 * LANES)

    def number(g, carry):
        at = pl.multiple_of(g * ROWS, ROWS)
        node = lane[pl.ds(at, ROWS), :]
        block = lax.shift_right_logical(node, 7)
        blk[pl.ds(at, ROWS), :] = jnp.take_along_axis(
            table, block, axis=1, mode="promise_in_bounds"
        )
        lane[pl.ds(at, ROWS), :] = lax.bitwise_and(node, LANES - 1)
        return carry

    lax.fori_loop(0, 3 * groups, number, 0)

    tall = lax.broadcasted_iota(jnp.int32, (LANES, LANES), 0)

    def heat(g, carry):
        at = pl.multiple_of(g * ROWS, ROWS)
        for j in range(ROWS):
            row = lane[pl.ds(at + j, 1), :]
            hot[:, pl.ds(pl.multiple_of((at + j) * LANES, LANES), LANES)] = jnp.where(
                row == tall, 1.0, 0.0
            ).astype(jnp.bfloat16)
        return carry

    lax.fori_loop(0, 3 * groups, heat, 0)

    def picked(source, count, first, value, index, block):
        for b in range(count):
            row = jnp.broadcast_to(source(b), (ROWS, LANES))
            got = jnp.take_along_axis(row, index, axis=1, mode="promise_in_bounds")
            value = jnp.where(block == first + b, got, value)
        return value

    def operate(t, source):
        def gather_own(g, carry):
            at = pl.multiple_of(g * ROWS, ROWS)
            index = lane[pl.ds(at, ROWS), :]
            block = blk[pl.ds(at, ROWS), :]
            vals[pl.ds(at, ROWS), :] = picked(
                lambda b: source[b : b + 1, :],
                own,
                0,
                jnp.zeros((ROWS, LANES), f32),
                index,
                block,
            )
            return carry

        lax.fori_loop(0, 3 * groups, gather_own, 0)

        for o in range(offsets):
            when_there(shifts[o], lambda o=o: fwd_copy(t, o).wait_recv())

        def gather_halo(g, carry):
            at = pl.multiple_of(g * ROWS, ROWS)
            u = [vals[pl.ds(at, ROWS), :]]
            for c in (1, 2):
                here = pl.multiple_of(c * rows + at, ROWS)
                u.append(
                    picked(
                        lambda b: fwd_in[t, b // slots, b % slots : b % slots + 1, :],
                        halo,
                        own,
                        vals[pl.ds(here, ROWS), :],
                        lane[pl.ds(here, ROWS), :],
                        blk[pl.ds(here, ROWS), :],
                    )
                )
            gx0, gy0, gx1, gy1 = [
                elem[pl.ds(pl.multiple_of(c * rows + at, ROWS), ROWS), :] for c in range(4)
            ]
            size = area[pl.ds(at, ROWS), :]
            scaled = depth[pl.ds(at, ROWS), :] * size
            third = size / 3.0
            from0, from1 = u[0] - u[2], u[1] - u[2]
            slope_x = scaled * (gx0 * from0 + gx1 * from1)
            slope_y = scaled * (gy0 * from0 + gy1 * from1)
            flow0 = gx0 * slope_x + gy0 * slope_y
            flow1 = gx1 * slope_x + gy1 * slope_y
            adds = [
                flow0 + third * u[0],
                flow1 + third * u[1],
                third * u[2] - (flow0 + flow1),
            ]
            for c in range(3):
                here = pl.multiple_of(c * rows + at, ROWS)
                top = adds[c].astype(jnp.bfloat16).astype(f32)
                hi[pl.ds(here, ROWS), :] = top
                lo[pl.ds(here, ROWS), :] = adds[c] - top
            return carry

        lax.fori_loop(0, groups, gather_halo, 0)

        def summed(first_group, last_group, count, first):
            names = first + lax.broadcasted_iota(jnp.int32, (count, LANES), 0)

            def body(g, acc):
                at = pl.multiple_of(g * ROWS, ROWS)
                parts = []
                for j in range(ROWS):
                    mask = blk[pl.ds(at + j, 1), :] == names
                    parts.append(
                        jnp.concatenate(
                            [
                                jnp.where(mask, hi[pl.ds(at + j, 1), :], 0.0),
                                jnp.where(mask, lo[pl.ds(at + j, 1), :], 0.0),
                            ],
                            axis=0,
                        ).astype(jnp.bfloat16)
                    )
                left = jnp.concatenate(parts, axis=1)
                right = hot[:, pl.ds(pl.multiple_of(at * LANES, LANES), ROWS * LANES)]
                return acc + lax.dot_general(
                    left, right, (((1,), (1,)), ((), ())), preferred_element_type=f32
                )

            acc = lax.fori_loop(
                first_group, last_group, body, jnp.zeros((2 * count, LANES), f32)
            )
            return acc[:count] + acc[count:]

        halo_sum = summed(groups, 3 * groups, halo, own)
        for o in range(offsets):
            bwd_out[t, o] = halo_sum[o * slots : (o + 1) * slots]
        for o in range(offsets):
            when_there(shifts[o], lambda o=o: bwd_copy(t, o).start())
        total = summed(0, 3 * groups, own, 0)
        for o in range(offsets):
            when_there(-shifts[o], lambda o=o: bwd_copy(t, o).wait_recv())
        names = lax.broadcasted_iota(jnp.int32, (own, LANES), 0)
        for o in range(offsets):
            for s in range(slots):
                total = total + jnp.where(
                    names == send[0, o, s], bwd_in[t, o, s : s + 1, :], 0.0
                )
        return total

    small = lax.broadcasted_iota(jnp.int32, (1, LANES), 1)

    def whole(a):
        return jnp.sum(jnp.sum(a, axis=0, keepdims=True), axis=1, keepdims=True)

    def start_sum(k, terms):
        line = jnp.zeros((1, LANES), f32)
        for i, term in enumerate(terms):
            line = jnp.where(small == i, whole(term), line)
        sum_out[k] = line
        sum_in[k, me] = line

        def push(i, carry):
            pltpu.make_async_remote_copy(
                src_ref=sum_out.at[k],
                dst_ref=sum_in.at[k, me],
                send_sem=sum_send_sem.at[k],
                recv_sem=sum_recv_sem.at[k],
                device_id=(lax.rem(me + i, n),),
                device_id_type=pl.DeviceIdType.MESH,
            ).start()
            return carry

        lax.fori_loop(1, n, push, 0)

    def sum_bytes(k):
        return sum_in.at[k, pl.ds(0, n - 1)]

    def finish_sum(k, count):
        pltpu.make_async_copy(sum_bytes(k), sum_bytes(k), sum_recv_sem.at[k]).wait()
        line = jnp.sum(sum_in[k], axis=0)
        return [
            jnp.sum(jnp.where(small == i, line, 0.0), axis=1, keepdims=True)
            for i in range(count)
        ]

    first_residual = forcing[...] - operate(0, guess)
    field[0] = first_residual
    pack(1, field.at[0])
    start_forward(1)
    image = operate(1, field.at[0])
    field[1] = image
    pack(2, field.at[1])
    start_forward(2)
    start_sum(0, [first_residual * first_residual, first_residual * image])
    image_two = operate(2, field.at[1])
    norm, crossed = finish_sum(0, 2)
    step = norm / crossed
    first_residual = field[0]
    image = field[1]
    second = first_residual - step * image
    applied = image - step * image_two
    start_sum(1, [second * second, second * applied, second * image, first_residual * applied])
    for t in range(3):
        for o in range(offsets):
            when_there(-shifts[o], lambda t=t, o=o: fwd_copy(t, o).wait_send())
            when_there(shifts[o], lambda t=t, o=o: bwd_copy(t, o).wait_send())
    fresh, own_pair, left_pair, right_pair = finish_sum(1, 4)
    beta = fresh / norm
    next_step = fresh / (own_pair + beta * (left_pair + right_pair) + beta * beta * crossed)
    elevation[...] = (
        guess[...] + step * first_residual + next_step * (second + beta * first_residual)
    )
    residual[...] = second - next_step * (applied + beta * image)
    for k in range(2):
        pltpu.make_async_copy(sum_bytes(k), sum_bytes(k), sum_send_sem.at[k]).wait()


def local(
    n,
    forcing,
    first_guess,
    corners,
    gradients,
    element_area,
    element_depth,
    send_blocks,
    recv_blocks,
):
    own, columns = forcing.shape
    _, offsets, slots = send_blocks.shape
    count = element_area.shape[0]
    rows = count // LANES
    assert columns == LANES and own + offsets * slots <= LANES and rows % ROWS == 0
    f32 = jnp.float32
    vmem = pl.BlockSpec(memory_space=pltpu.VMEM)
    smem = pl.BlockSpec(memory_space=pltpu.SMEM)
    dma = pltpu.SemaphoreType.DMA
    part = (3, offsets, slots, LANES)
    return pl.pallas_call(
        functools.partial(kernel, n),
        out_shape=(jax.ShapeDtypeStruct((own, columns), f32),) * 2,
        in_specs=[vmem] * 6 + [smem] * 2,
        out_specs=(vmem, vmem),
        scratch_shapes=[
            pltpu.VMEM((3 * rows, LANES), jnp.int32),
            pltpu.VMEM((3 * rows, LANES), jnp.int32),
            pltpu.VMEM((LANES, 3 * count), jnp.bfloat16),
            pltpu.VMEM((4 * rows, LANES), f32),
            pltpu.VMEM((3 * rows, LANES), f32),
            pltpu.VMEM((3 * rows, LANES), f32),
            pltpu.VMEM((3 * rows, LANES), f32),
            pltpu.VMEM((2, own, LANES), f32),
            pltpu.VMEM((offsets * slots, LANES), f32),
            pltpu.VMEM(part, f32),
            pltpu.VMEM(part, f32),
            pltpu.VMEM(part, f32),
            pltpu.VMEM(part, f32),
            pltpu.VMEM((2, 1, LANES), f32),
            pltpu.VMEM((2, n, 1, LANES), f32),
            dma((3, offsets)),
            dma((3, offsets)),
            dma((3, offsets)),
            dma((3, offsets)),
            dma((2,)),
            dma((2,)),
        ],
        compiler_params=pltpu.CompilerParams(collective_id=0, has_side_effects=True),
    )(
        forcing,
        first_guess,
        corners,
        gradients,
        element_area.reshape(rows, LANES),
        element_depth.reshape(rows, LANES),
        send_blocks,
        recv_blocks,
    )


def solution(mesh):
    placed = (
        P("dom", None),
        P("dom", None),
        P(None, "dom"),
        P(None, "dom"),
        P("dom"),
        P("dom"),
        P("dom", None, None),
        P("dom", None, None),
    )
    return jax.shard_map(
        functools.partial(local, mesh.shape["dom"]),
        mesh=mesh,
        in_specs=placed,
        out_specs=(P("dom", None), P("dom", None)),
        check_vma=False,
    )
```

```python
import functools

import jax
import jax.numpy as jnp
from jax import lax
from jax.experimental import pallas as pl
from jax.experimental.pallas import tpu as pltpu
from jax.sharding import PartitionSpec as P

LANES = 128
ROWS = 8
WIDE = 4


def shift_list(offsets):
    half_count = offsets // 2
    return [
        shift_at - half_count if shift_at < half_count else shift_at - half_count + 1
        for shift_at in range(offsets)
    ]


def learning_rounds(n, reach):
    rounds = []
    while reach < n - 1:
        rounds.append(reach)
        reach *= 2
    return rounds


def kernel(
    n,
    forcing,
    guess,
    corners,
    gradients,
    area,
    depth,
    send,
    recv,
    elevation,
    residual,
    blk,
    lane,
    hot,
    elem,
    vals,
    hi,
    lo,
    field,
    halo_part,
    fwd_out,
    fwd_in,
    bwd_out,
    bwd_in,
    sum_out,
    sum_in,
    fwd_send_sem,
    fwd_recv_sem,
    bwd_send_sem,
    bwd_recv_sem,
    sum_send_sem,
    sum_recv_sem,
    known,
):
    own, _ = forcing.shape
    _, offsets, slots = send.shape
    halo = offsets * slots
    rows = area.shape[0]
    groups = rows // ROWS
    shifts = shift_list(offsets)
    me = lax.axis_index("dom")
    f32 = jnp.float32

    def there(distance):
        return jnp.logical_and(me + distance >= 0, me + distance < n)

    def fwd_copy(t, o):
        return pltpu.make_async_remote_copy(
            src_ref=fwd_out.at[t, o],
            dst_ref=fwd_in.at[t, o],
            send_sem=fwd_send_sem.at[t, o],
            recv_sem=fwd_recv_sem.at[t, o],
            device_id=(me - shifts[o],),
            device_id_type=pl.DeviceIdType.MESH,
        )

    def bwd_copy(t, o):
        return pltpu.make_async_remote_copy(
            src_ref=bwd_out.at[t, o],
            dst_ref=bwd_in.at[t, o],
            send_sem=bwd_send_sem.at[t, o],
            recv_sem=bwd_recv_sem.at[t, o],
            device_id=(me + shifts[o],),
            device_id_type=pl.DeviceIdType.MESH,
        )

    def when_there(distance, action):
        @pl.when(there(distance))
        def _():
            action()

    barrier = pltpu.get_barrier_semaphore()
    reach = max(shifts)
    near = [shift for shift in range(-reach, reach + 1) if shift != 0]
    for shift in near:
        when_there(
            shift,
            lambda shift=shift: pl.semaphore_signal(
                barrier,
                inc=1,
                device_id=(me + shift,),
                device_id_type=pl.DeviceIdType.MESH,
            ),
        )

    rounds = learning_rounds(n, reach)

    def tell(i):
        for side in range(2):
            far = rounds[i] * (2 * side - 1)
            when_there(
                far,
                lambda side=side, far=far: pl.semaphore_signal(
                    known.at[i, side],
                    inc=1,
                    device_id=(me + far,),
                    device_id_type=pl.DeviceIdType.MESH,
                ),
            )

    def learn(i):
        for side in range(2):
            far = rounds[i] * (1 - 2 * side)
            when_there(
                far, lambda side=side: pl.semaphore_wait(known.at[i, side], 1)
            )

    def next_round(i):
        if i > 0 and i <= len(rounds):
            learn(i - 1)
        if i < len(rounds):
            tell(i)

    for o in range(offsets):

        @pl.when(jnp.logical_not(there(shifts[o])))
        def _():
            for t in range(3):
                fwd_in[t, o] = jnp.zeros((slots, LANES), f32)

        @pl.when(jnp.logical_not(there(-shifts[o])))
        def _():
            for t in range(3):
                bwd_in[t, o] = jnp.zeros((slots, LANES), f32)

    def pack(t, source):
        for o in range(offsets):
            for s in range(slots):
                at = jnp.minimum(send[0, o, s], own - 1)
                fwd_out[t, o, s : s + 1, :] = source[pl.ds(at, 1), :]

    def start_forward(t):
        for o in range(offsets):
            when_there(-shifts[o], lambda o=o: fwd_copy(t, o).start())

    def lay(r, carry):
        at = pl.multiple_of(r * LANES, LANES)
        for c in range(3):
            lane[pl.ds(c * rows + r, 1), :] = corners[c : c + 1, pl.ds(at, LANES)]
        for c in range(4):
            elem[pl.ds(c * rows + r, 1), :] = gradients[c : c + 1, pl.ds(at, LANES)]
        return carry

    lax.fori_loop(0, rows, lay, 0)

    wide = lax.broadcasted_iota(jnp.int32, (ROWS, LANES), 1)
    table = jnp.where(wide < own, wide, 2 * LANES)
    for o in range(offsets):
        for s in range(slots):
            table = jnp.where(wide == own + recv[0, o, s], own + o * slots + s, table)
    table = jnp.where(wide < own + halo, table, 2 * LANES)

    def number(g, carry):
        at = pl.multiple_of(g * ROWS, ROWS)
        node = lane[pl.ds(at, ROWS), :]
        block = lax.shift_right_logical(node, 7)
        blk[pl.ds(at, ROWS), :] = jnp.take_along_axis(
            table, block, axis=1, mode="promise_in_bounds"
        )
        lane[pl.ds(at, ROWS), :] = lax.bitwise_and(node, LANES - 1)
        return carry

    lax.fori_loop(0, 3 * groups, number, 0)

    tall = lax.broadcasted_iota(jnp.int32, (LANES, LANES), 0)

    def heat(g, carry):
        at = pl.multiple_of(g * ROWS, ROWS)
        for j in range(ROWS):
            row = lane[pl.ds(at + j, 1), :]
            hot[pl.ds(pl.multiple_of((at + j) * LANES, LANES), LANES), :] = (
                jnp.where(row == tall, 1.0, 0.0).T.astype(jnp.bfloat16)
            )
        return carry

    half = 3 * groups // 2
    lax.fori_loop(0, half, heat, 0)
    pack(0, guess)
    pl.semaphore_wait(
        barrier, jnp.minimum(me, reach) + jnp.minimum(n - 1 - me, reach)
    )
    start_forward(0)
    next_round(0)
    lax.fori_loop(half, 3 * groups, heat, 0)

    def picked(source, count, first, value, index, block):
        for b in range(count):
            row = jnp.broadcast_to(source(b), (ROWS, LANES))
            got = jnp.take_along_axis(row, index, axis=1, mode="promise_in_bounds")
            value = jnp.where(block == first + b, got, value)
        return value

    def operate(t, source, between):
        def gather_own(g, carry):
            for j in range(WIDE):
                at = pl.multiple_of((g * WIDE + j) * ROWS, ROWS)
                vals[pl.ds(at, ROWS), :] = picked(
                    lambda b: source[b : b + 1, :],
                    own,
                    0,
                    jnp.zeros((ROWS, LANES), f32),
                    lane[pl.ds(at, ROWS), :],
                    blk[pl.ds(at, ROWS), :],
                )
            return carry

        lax.fori_loop(0, 3 * groups // WIDE, gather_own, 0)
        for o in range(offsets):
            when_there(shifts[o], lambda o=o: fwd_copy(t, o).wait_recv())

        def one_group(g, energy):
            at = pl.multiple_of(g * ROWS, ROWS)
            u = [vals[pl.ds(at, ROWS), :]]
            for c in (1, 2):
                here = pl.multiple_of(c * rows + at, ROWS)
                u.append(
                    picked(
                        lambda b: fwd_in[t, b // slots, b % slots : b % slots + 1, :],
                        halo,
                        own,
                        vals[pl.ds(here, ROWS), :],
                        lane[pl.ds(here, ROWS), :],
                        blk[pl.ds(here, ROWS), :],
                    )
                )
            gx0, gy0, gx1, gy1 = [
                elem[pl.ds(pl.multiple_of(c * rows + at, ROWS), ROWS), :] for c in range(4)
            ]
            size = area[pl.ds(at, ROWS), :]
            scaled = depth[pl.ds(at, ROWS), :] * size
            third = size / 3.0
            from0, from1 = u[0] - u[2], u[1] - u[2]
            slope_x = scaled * (gx0 * from0 + gx1 * from1)
            slope_y = scaled * (gy0 * from0 + gy1 * from1)
            flow0 = gx0 * slope_x + gy0 * slope_y
            flow1 = gx1 * slope_x + gy1 * slope_y
            adds = [
                flow0 + third * u[0],
                flow1 + third * u[1],
                third * u[2] - (flow0 + flow1),
            ]
            for c in range(3):
                here = pl.multiple_of(c * rows + at, ROWS)
                top = adds[c].astype(jnp.bfloat16).astype(f32)
                hi[pl.ds(here, ROWS), :] = top
                lo[pl.ds(here, ROWS), :] = adds[c] - top
            return energy + (
                slope_x * (gx0 * from0 + gx1 * from1)
                + slope_y * (gy0 * from0 + gy1 * from1)
                + third * (u[0] * u[0] + u[1] * u[1] + u[2] * u[2])
            )

        def gather_halo(g, energy):
            for j in range(2):
                energy = one_group(g * 2 + j, energy)
            return energy

        energy = lax.fori_loop(0, groups // 2, gather_halo, jnp.zeros((ROWS, LANES), f32))
        between(energy)

        def summed(first_group, last_group, count, first):
            names = first + lax.broadcasted_iota(jnp.int32, (count, LANES), 0)

            def body(g, acc):
                at = pl.multiple_of(g * WIDE * ROWS, ROWS)
                parts = []
                for j in range(WIDE * ROWS):
                    mask = blk[pl.ds(at + j, 1), :] == names
                    parts.append(
                        jnp.concatenate(
                            [
                                jnp.where(mask, hi[pl.ds(at + j, 1), :], 0.0),
                                jnp.where(mask, lo[pl.ds(at + j, 1), :], 0.0),
                            ],
                            axis=0,
                        ).astype(jnp.bfloat16)
                    )
                left = jnp.concatenate(parts, axis=1)
                right = hot[pl.ds(pl.multiple_of(at * LANES, LANES), WIDE * ROWS * LANES), :]
                return acc + jnp.dot(left, right, preferred_element_type=f32)

            acc = lax.fori_loop(
                first_group // WIDE, last_group // WIDE, body, jnp.zeros((2 * count, LANES), f32)
            )
            return acc[:count] + acc[count:]

        if t == 0:
            next_round(1)
        halo_sum = summed(groups, 3 * groups, halo, own)
        for o in range(offsets):
            bwd_out[t, o] = halo_sum[o * slots : (o + 1) * slots]
        for o in range(offsets):
            when_there(shifts[o], lambda o=o: bwd_copy(t, o).start())
        if t == 0:
            next_round(2)
        total = summed(0, 3 * groups, own, 0)
        for o in range(offsets):
            when_there(-shifts[o], lambda o=o: bwd_copy(t, o).wait_recv())
        names = lax.broadcasted_iota(jnp.int32, (own, LANES), 0)
        for o in range(offsets):
            for s in range(slots):
                total = total + jnp.where(
                    names == send[0, o, s], bwd_in[t, o, s : s + 1, :], 0.0
                )
        return total

    small = lax.broadcasted_iota(jnp.int32, (1, LANES), 1)

    def whole(a):
        return jnp.sum(jnp.sum(a, axis=0, keepdims=True), axis=1, keepdims=True)

    def start_sum(k, terms):
        line = jnp.zeros((1, LANES), f32)
        for i, term in enumerate(terms):
            line = jnp.where(small == i, whole(term), line)
        sum_out[k] = line
        sum_in[k, me] = line

        def push(i, carry):
            pltpu.make_async_remote_copy(
                src_ref=sum_out.at[k],
                dst_ref=sum_in.at[k, me],
                send_sem=sum_send_sem.at[k],
                recv_sem=sum_recv_sem.at[k],
                device_id=(lax.rem(me + i, n),),
                device_id_type=pl.DeviceIdType.MESH,
            ).start()
            return carry

        lax.fori_loop(1, n, push, 0)

    def sum_bytes(k):
        return sum_in.at[k, pl.ds(0, n - 1)]

    def finish_sum(k, count):
        pltpu.make_async_copy(sum_bytes(k), sum_bytes(k), sum_recv_sem.at[k]).wait()
        line = jnp.sum(sum_in[k], axis=0)
        return [
            jnp.sum(jnp.where(small == i, line, 0.0), axis=1, keepdims=True)
            for i in range(count)
        ]

    field[0] = forcing[...] - operate(0, guess, lambda energy: None)
    pack(1, field.at[0])
    start_forward(1)

    next_round(3)

    def first_sums(energy):
        for i in range(4, len(rounds) + 1):
            next_round(i)
        start_sum(0, [field[0] * field[0], energy])

    image = operate(1, field.at[0], first_sums)
    norm, crossed = finish_sum(0, 2)
    step = norm / crossed
    field[1] = field[0] - step * image
    pack(2, field.at[1])
    start_forward(2)
    field[2] = image

    def second_sums(energy):
        start_sum(1, [field[1] * field[1], energy, field[1] * field[2]])

    applied = operate(2, field.at[1], second_sums)
    for t in range(3):
        for o in range(offsets):
            when_there(-shifts[o], lambda t=t, o=o: fwd_copy(t, o).wait_send())
            when_there(shifts[o], lambda t=t, o=o: bwd_copy(t, o).wait_send())
    fresh, own_pair, mixed = finish_sum(1, 3)
    beta = fresh / norm
    next_step = fresh / (own_pair + beta * (2.0 * mixed + beta * crossed))
    elevation[...] = guess[...] + step * field[0] + next_step * (field[1] + beta * field[0])
    residual[...] = field[1] - next_step * (applied + beta * field[2])
    for k in range(2):
        pltpu.make_async_copy(sum_bytes(k), sum_bytes(k), sum_send_sem.at[k]).wait()


def local(
    n,
    forcing,
    first_guess,
    corners,
    gradients,
    element_area,
    element_depth,
    send_blocks,
    recv_blocks,
):
    own, columns = forcing.shape
    _, offsets, slots = send_blocks.shape
    count = element_area.shape[0]
    rows = count // LANES
    assert columns == LANES and own + offsets * slots <= LANES and rows % (ROWS * WIDE) == 0
    f32 = jnp.float32
    vmem = pl.BlockSpec(memory_space=pltpu.VMEM)
    smem = pl.BlockSpec(memory_space=pltpu.SMEM)
    dma = pltpu.SemaphoreType.DMA
    part = (3, offsets, slots, LANES)
    return pl.pallas_call(
        functools.partial(kernel, n),
        out_shape=(jax.ShapeDtypeStruct((own, columns), f32),) * 2,
        in_specs=[vmem] * 6 + [smem] * 2,
        out_specs=(vmem, vmem),
        scratch_shapes=[
            pltpu.VMEM((3 * rows, LANES), jnp.int32),
            pltpu.VMEM((3 * rows, LANES), jnp.int32),
            pltpu.VMEM((3 * count, LANES), jnp.bfloat16),
            pltpu.VMEM((4 * rows, LANES), f32),
            pltpu.VMEM((3 * rows, LANES), f32),
            pltpu.VMEM((3 * rows, LANES), f32),
            pltpu.VMEM((3 * rows, LANES), f32),
            pltpu.VMEM((3, own, LANES), f32),
            pltpu.VMEM((offsets * slots, LANES), f32),
            pltpu.VMEM(part, f32),
            pltpu.VMEM(part, f32),
            pltpu.VMEM(part, f32),
            pltpu.VMEM(part, f32),
            pltpu.VMEM((2, 1, LANES), f32),
            pltpu.VMEM((2, n, 1, LANES), f32),
            dma((3, offsets)),
            dma((3, offsets)),
            dma((3, offsets)),
            dma((3, offsets)),
            dma((2,)),
            dma((2,)),
            pltpu.SemaphoreType.REGULAR((len(learning_rounds(n, max(shift_list(offsets)))) + 1, 2)),
        ],
        compiler_params=pltpu.CompilerParams(collective_id=0, has_side_effects=True),
    )(
        forcing,
        first_guess,
        corners,
        gradients,
        element_area.reshape(rows, LANES),
        element_depth.reshape(rows, LANES),
        send_blocks,
        recv_blocks,
    )


def solution(mesh):
    placed = (
        P("dom", None),
        P("dom", None),
        P(None, "dom"),
        P(None, "dom"),
        P("dom"),
        P("dom"),
        P("dom", None, None),
        P("dom", None, None),
    )
    return jax.shard_map(
        functools.partial(local, mesh.shape["dom"]),
        mesh=mesh,
        in_specs=placed,
        out_specs=(P("dom", None), P("dom", None)),
        check_vma=False,
    )
```

```python
import functools

import jax
import jax.numpy as jnp
from jax import lax
from jax.experimental import pallas as pl
from jax.experimental.pallas import tpu as pltpu
from jax.sharding import PartitionSpec as P

LANES = 128
ROWS = 8
WIDE = 4


def shift_list(offsets):
    half_count = offsets // 2
    return [
        shift_at - half_count if shift_at < half_count else shift_at - half_count + 1
        for shift_at in range(offsets)
    ]


def learning_rounds(n, reach):
    rounds = []
    while reach < n - 1:
        rounds.append(reach)
        reach *= 2
    return rounds


def kernel(
    n,
    forcing,
    guess,
    corners,
    gradients,
    area,
    depth,
    send,
    recv,
    both,
    blk,
    lane,
    hot,
    elem,
    vals,
    hi,
    lo,
    field,
    halo_part,
    fwd_out,
    fwd_in,
    bwd_out,
    bwd_in,
    sum_out,
    sum_in,
    fwd_send_sem,
    fwd_recv_sem,
    bwd_send_sem,
    bwd_recv_sem,
    sum_send_sem,
    sum_recv_sem,
    known,
):
    own, _ = forcing.shape
    _, offsets, slots = send.shape
    halo = offsets * slots
    rows = area.shape[0]
    groups = rows // ROWS
    shifts = shift_list(offsets)
    me = lax.axis_index("dom")
    f32 = jnp.float32

    def there(distance):
        return jnp.logical_and(me + distance >= 0, me + distance < n)

    def fwd_copy(t, o):
        return pltpu.make_async_remote_copy(
            src_ref=fwd_out.at[t, o],
            dst_ref=fwd_in.at[t, o],
            send_sem=fwd_send_sem.at[t, o],
            recv_sem=fwd_recv_sem.at[t, o],
            device_id=(me - shifts[o],),
            device_id_type=pl.DeviceIdType.MESH,
        )

    def bwd_copy(t, o):
        return pltpu.make_async_remote_copy(
            src_ref=bwd_out.at[t, o],
            dst_ref=bwd_in.at[t, o],
            send_sem=bwd_send_sem.at[t, o],
            recv_sem=bwd_recv_sem.at[t, o],
            device_id=(me + shifts[o],),
            device_id_type=pl.DeviceIdType.MESH,
        )

    def when_there(distance, action):
        @pl.when(there(distance))
        def _():
            action()

    barrier = pltpu.get_barrier_semaphore()
    reach = max(shifts)
    near = [shift for shift in range(-reach, reach + 1) if shift != 0]
    for shift in near:
        when_there(
            shift,
            lambda shift=shift: pl.semaphore_signal(
                barrier,
                inc=1,
                device_id=(me + shift,),
                device_id_type=pl.DeviceIdType.MESH,
            ),
        )

    rounds = learning_rounds(n, reach)

    def tell(i):
        for side in range(2):
            far = rounds[i] * (2 * side - 1)
            when_there(
                far,
                lambda side=side, far=far: pl.semaphore_signal(
                    known.at[i, side],
                    inc=1,
                    device_id=(me + far,),
                    device_id_type=pl.DeviceIdType.MESH,
                ),
            )

    def learn(i):
        for side in range(2):
            far = rounds[i] * (1 - 2 * side)
            when_there(
                far, lambda side=side: pl.semaphore_wait(known.at[i, side], 1)
            )

    def next_round(i):
        if i > 0 and i <= len(rounds):
            learn(i - 1)
        if i < len(rounds):
            tell(i)

    for o in range(offsets):

        @pl.when(jnp.logical_not(there(shifts[o])))
        def _():
            for t in range(3):
                fwd_in[t, o] = jnp.zeros((slots, LANES), f32)

        @pl.when(jnp.logical_not(there(-shifts[o])))
        def _():
            for t in range(3):
                bwd_in[t, o] = jnp.zeros((slots, LANES), f32)

    def pack(t, source):
        for o in range(offsets):
            for s in range(slots):
                at = jnp.minimum(send[0, o, s], own - 1)
                fwd_out[t, o, s : s + 1, :] = source[pl.ds(at, 1), :]

    def start_forward(t):
        for o in range(offsets):
            when_there(-shifts[o], lambda o=o: fwd_copy(t, o).start())

    def lay(r, carry):
        at = pl.multiple_of(r * LANES, LANES)
        for c in range(3):
            lane[pl.ds(c * rows + r, 1), :] = corners[c : c + 1, pl.ds(at, LANES)]
        for c in range(4):
            elem[pl.ds(c * rows + r, 1), :] = gradients[c : c + 1, pl.ds(at, LANES)]
        return carry

    lax.fori_loop(0, rows, lay, 0)

    wide = lax.broadcasted_iota(jnp.int32, (ROWS, LANES), 1)
    table = jnp.where(wide < own, wide, 2 * LANES)
    for o in range(offsets):
        for s in range(slots):
            table = jnp.where(wide == own + recv[0, o, s], own + o * slots + s, table)
    table = jnp.where(wide < own + halo, table, 2 * LANES)

    def number(g, carry):
        at = pl.multiple_of(g * ROWS, ROWS)
        node = lane[pl.ds(at, ROWS), :]
        block = lax.shift_right_logical(node, 7)
        blk[pl.ds(at, ROWS), :] = jnp.take_along_axis(
            table, block, axis=1, mode="promise_in_bounds"
        )
        lane[pl.ds(at, ROWS), :] = lax.bitwise_and(node, LANES - 1)
        return carry

    lax.fori_loop(0, 3 * groups, number, 0)

    tall = lax.broadcasted_iota(jnp.int32, (LANES, LANES), 0)

    def heat(g, carry):
        at = pl.multiple_of(g * ROWS, ROWS)
        for j in range(ROWS):
            row = lane[pl.ds(at + j, 1), :]
            hot[pl.ds(pl.multiple_of((at + j) * LANES, LANES), LANES), :] = (
                jnp.where(row == tall, 1.0, 0.0).T.astype(jnp.bfloat16)
            )
        return carry

    lax.fori_loop(groups, 2 * groups, heat, 0)
    pack(0, guess)
    pl.semaphore_wait(
        barrier, jnp.minimum(me, reach) + jnp.minimum(n - 1 - me, reach)
    )
    start_forward(0)
    next_round(0)
    lax.fori_loop(2 * groups, 3 * groups, heat, 0)

    def picked(source, count, first, value, index, block):
        for b in range(count):
            row = jnp.broadcast_to(source(b), (ROWS, LANES))
            got = jnp.take_along_axis(row, index, axis=1, mode="promise_in_bounds")
            value = jnp.where(block == first + b, got, value)
        return value

    def operate(t, source, between, after, finished):
        def gather_own(g, carry):
            for j in range(WIDE):
                at = pl.multiple_of((g * WIDE + j) * ROWS, ROWS)
                vals[t // 2, pl.ds(at, ROWS), :] = picked(
                    lambda b: source[b : b + 1, :],
                    own,
                    0,
                    jnp.zeros((ROWS, LANES), f32),
                    lane[pl.ds(at, ROWS), :],
                    blk[pl.ds(at, ROWS), :],
                )
            return carry

        lax.fori_loop(0, 3 * groups // WIDE, gather_own, 0)
        for o in range(offsets):
            when_there(shifts[o], lambda o=o: fwd_copy(t, o).wait_recv())

        step = finished()

        def one_group(g, energy):
            at = pl.multiple_of(g * ROWS, ROWS)
            u = [vals[t // 2, pl.ds(at, ROWS), :]]
            for c in (1, 2):
                here = pl.multiple_of(c * rows + at, ROWS)
                u.append(
                    picked(
                        lambda b: fwd_in[t, b // slots, b % slots : b % slots + 1, :],
                        halo,
                        own,
                        vals[t // 2, pl.ds(here, ROWS), :],
                        lane[pl.ds(here, ROWS), :],
                        blk[pl.ds(here, ROWS), :],
                    )
                )
                if t == 1:
                    vals[0, pl.ds(here, ROWS), :] = u[c]
            if t == 2:
                for c in range(3):
                    here = pl.multiple_of(c * rows + at, ROWS)
                    u[c] = vals[0, pl.ds(here, ROWS), :] - step * u[c]
            gx0, gy0, gx1, gy1 = [
                elem[pl.ds(pl.multiple_of(c * rows + at, ROWS), ROWS), :] for c in range(4)
            ]
            size = area[pl.ds(at, ROWS), :]
            scaled = depth[pl.ds(at, ROWS), :] * size
            third = size / 3.0
            from0, from1 = u[0] - u[2], u[1] - u[2]
            slope_x = scaled * (gx0 * from0 + gx1 * from1)
            slope_y = scaled * (gy0 * from0 + gy1 * from1)
            flow0 = gx0 * slope_x + gy0 * slope_y
            flow1 = gx1 * slope_x + gy1 * slope_y
            adds = [
                flow0 + third * u[0],
                flow1 + third * u[1],
                third * u[2] - (flow0 + flow1),
            ]
            for c in range(3):
                here = pl.multiple_of(c * rows + at, ROWS)
                top = adds[c].astype(jnp.bfloat16).astype(f32)
                hi[pl.ds(here, ROWS), :] = top
                lo[pl.ds(here, ROWS), :] = adds[c] - top
            return energy + (
                slope_x * (gx0 * from0 + gx1 * from1)
                + slope_y * (gy0 * from0 + gy1 * from1)
                + third * (u[0] * u[0] + u[1] * u[1] + u[2] * u[2])
            )

        def gather_halo(g, energy):
            for j in range(2):
                energy = one_group(g * 2 + j, energy)
            return energy

        energy = lax.fori_loop(0, groups // 2, gather_halo, jnp.zeros((ROWS, LANES), f32))
        between(energy)

        def summed(first_group, last_group, count, first):
            names = first + lax.broadcasted_iota(jnp.int32, (count, LANES), 0)

            def body(g, acc):
                at = pl.multiple_of(g * WIDE * ROWS, ROWS)
                parts = []
                for j in range(WIDE * ROWS):
                    mask = blk[pl.ds(at + j, 1), :] == names
                    parts.append(
                        jnp.concatenate(
                            [
                                jnp.where(mask, hi[pl.ds(at + j, 1), :], 0.0),
                                jnp.where(mask, lo[pl.ds(at + j, 1), :], 0.0),
                            ],
                            axis=0,
                        ).astype(jnp.bfloat16)
                    )
                left = jnp.concatenate(parts, axis=1)
                right = hot[pl.ds(pl.multiple_of(at * LANES, LANES), WIDE * ROWS * LANES), :]
                return acc + jnp.dot(left, right, preferred_element_type=f32)

            acc = lax.fori_loop(
                first_group // WIDE, last_group // WIDE, body, jnp.zeros((2 * count, LANES), f32)
            )
            return acc[:count] + acc[count:]

        if t == 0:
            next_round(1)
        halo_sum = summed(groups, 3 * groups, halo, own)
        for o in range(offsets):
            bwd_out[t, o] = halo_sum[o * slots : (o + 1) * slots]
        for o in range(offsets):
            when_there(shifts[o], lambda o=o: bwd_copy(t, o).start())
        after()
        if t == 0:
            next_round(2)
            lax.fori_loop(0, groups, heat, 0)
        total = summed(0, 3 * groups, own, 0)
        for o in range(offsets):
            when_there(-shifts[o], lambda o=o: bwd_copy(t, o).wait_recv())
        names = lax.broadcasted_iota(jnp.int32, (own, LANES), 0)
        for o in range(offsets):
            for s in range(slots):
                total = total + jnp.where(
                    names == send[0, o, s], bwd_in[t, o, s : s + 1, :], 0.0
                )
        return total

    small = lax.broadcasted_iota(jnp.int32, (1, LANES), 1)

    def whole(a):
        return jnp.sum(jnp.sum(a, axis=0, keepdims=True), axis=1, keepdims=True)

    def start_sum(k, terms):
        line = jnp.zeros((1, LANES), f32)
        for i, term in enumerate(terms):
            line = jnp.where(small == i, whole(term), line)
        sum_out[k] = line
        sum_in[k, me] = line

        def push(i, carry):
            pltpu.make_async_remote_copy(
                src_ref=sum_out.at[k],
                dst_ref=sum_in.at[k, me],
                send_sem=sum_send_sem.at[k],
                recv_sem=sum_recv_sem.at[k],
                device_id=(lax.rem(me + i, n),),
                device_id_type=pl.DeviceIdType.MESH,
            ).start()
            return carry

        lax.fori_loop(1, n, push, 0)

    def sum_bytes(k):
        return sum_in.at[k, pl.ds(0, n - 1)]

    def finish_sum(k, count):
        pltpu.make_async_copy(sum_bytes(k), sum_bytes(k), sum_recv_sem.at[k]).wait()
        line = jnp.sum(sum_in[k], axis=0)
        return [
            jnp.sum(jnp.where(small == i, line, 0.0), axis=1, keepdims=True)
            for i in range(count)
        ]

    def nothing(*_):
        return None

    field[0] = forcing[...] - operate(0, guess, nothing, nothing, nothing)
    pack(1, field.at[0])
    start_forward(1)
    next_round(3)
    for i in range(4, len(rounds) + 1):
        next_round(i)
    energies = []

    def first_sums():
        start_sum(0, [field[0] * field[0], energies[0]])

    field[2] = operate(1, field.at[0], energies.append, first_sums, nothing)
    pack(2, field.at[2])
    start_forward(2)
    sums = []

    def first_step():
        norm, crossed = finish_sum(0, 2)
        step = norm / crossed
        sums.extend([norm, crossed, step])
        field[1] = field[0] - step * field[2]
        return step

    def second_sums(energy):
        start_sum(1, [field[1] * field[1], energy, field[1] * field[2]])

    applied = operate(2, field.at[2], second_sums, nothing, first_step)
    norm, crossed, step = sums
    for t in range(3):
        for o in range(offsets):
            when_there(-shifts[o], lambda t=t, o=o: fwd_copy(t, o).wait_send())
            when_there(shifts[o], lambda t=t, o=o: bwd_copy(t, o).wait_send())
    fresh, own_pair, mixed = finish_sum(1, 3)
    beta = fresh / norm
    next_step = fresh / (own_pair + beta * (2.0 * mixed + beta * crossed))
    both[0:own] = guess[...] + step * field[0] + next_step * (field[1] + beta * field[0])
    both[own : 2 * own] = field[1] - next_step * (applied + beta * field[2])
    for k in range(2):
        pltpu.make_async_copy(sum_bytes(k), sum_bytes(k), sum_send_sem.at[k]).wait()


def local(
    n,
    forcing,
    first_guess,
    corners,
    gradients,
    element_area,
    element_depth,
    send_blocks,
    recv_blocks,
):
    own, columns = forcing.shape
    _, offsets, slots = send_blocks.shape
    count = element_area.shape[0]
    rows = count // LANES
    assert columns == LANES and own + offsets * slots <= LANES and rows % (ROWS * WIDE) == 0
    f32 = jnp.float32
    vmem = pl.BlockSpec(memory_space=pltpu.VMEM)
    smem = pl.BlockSpec(memory_space=pltpu.SMEM)
    dma = pltpu.SemaphoreType.DMA
    part = (3, offsets, slots, LANES)
    both = pl.pallas_call(
        functools.partial(kernel, n),
        out_shape=jax.ShapeDtypeStruct((2 * own, columns), f32),
        in_specs=[vmem] * 6 + [smem] * 2,
        out_specs=vmem,
        scratch_shapes=[
            pltpu.VMEM((3 * rows, LANES), jnp.int32),
            pltpu.VMEM((3 * rows, LANES), jnp.int32),
            pltpu.VMEM((3 * count, LANES), jnp.bfloat16),
            pltpu.VMEM((4 * rows, LANES), f32),
            pltpu.VMEM((2, 3 * rows, LANES), f32),
            pltpu.VMEM((3 * rows, LANES), f32),
            pltpu.VMEM((3 * rows, LANES), f32),
            pltpu.VMEM((3, own, LANES), f32),
            pltpu.VMEM((offsets * slots, LANES), f32),
            pltpu.VMEM(part, f32),
            pltpu.VMEM(part, f32),
            pltpu.VMEM(part, f32),
            pltpu.VMEM(part, f32),
            pltpu.VMEM((2, 1, LANES), f32),
            pltpu.VMEM((2, n, 1, LANES), f32),
            dma((3, offsets)),
            dma((3, offsets)),
            dma((3, offsets)),
            dma((3, offsets)),
            dma((2,)),
            dma((2,)),
            pltpu.SemaphoreType.REGULAR((len(learning_rounds(n, max(shift_list(offsets)))) + 1, 2)),
        ],
        compiler_params=pltpu.CompilerParams(collective_id=0, has_side_effects=True),
    )(
        forcing,
        first_guess,
        corners,
        gradients,
        element_area.reshape(rows, LANES),
        element_depth.reshape(rows, LANES),
        send_blocks,
        recv_blocks,
    )
    return both[:own], both[own:]


def solution(mesh):
    placed = (
        P("dom", None),
        P("dom", None),
        P(None, "dom"),
        P(None, "dom"),
        P("dom"),
        P("dom"),
        P("dom", None, None),
        P("dom", None, None),
    )
    return jax.shard_map(
        functools.partial(local, mesh.shape["dom"]),
        mesh=mesh,
        in_specs=placed,
        out_specs=(P("dom", None), P("dom", None)),
        check_vma=False,
    )
```
